32 devices in a mesh: island: 4 (over z), tp: 8 (over y, x, core).
Axes of the slice: x: 2, y: 2, z: 4, core: 2. Of those that a mesh axis runs over, the one named last changes fastest.
Arguments:
- tokens: bfloat16 [4, 256, 4096], P('island', 'tp'), may hold values from -6 to 6
- cotangent: bfloat16 [4, 256, 4096], P('island', 'tp'), may hold values from -1.5 to 1.5
- gate_weight: bfloat16 [4096, 7168], P(None, 'tp'), may hold values from -0.09375 to 0.09375
- up_weight: bfloat16 [4096, 7168], P(None, 'tp'), may hold values from -0.09375 to 0.09375
- down_weight: bfloat16 [7168, 4096], P('tp'), may hold values from -0.0625 to 0.0625
- local_fragment: float32 [4, 196608], P('island', 'tp'), may hold values from -9 to 9
- global_fragment: float32 [196608], P('tp'), may hold values from -6 to 6
- outer_velocity: float32 [196608], P('tp'), may hold values from -3 to 3
Outputs:
- layer_out: bfloat16 [4, 256, 4096], P('island', 'tp')
- input_grad: bfloat16 [4, 256, 4096], P('island', 'tp')
- new_fragment: float32 [196608], P('tp')
- new_velocity: float32 [196608], P('tp')
The draws below stay inside these ranges and needn't reach their ends.
All inputs are finite; a program needn't handle non-finite values.
Results may differ from the reference program's by a relative error of at most 0.015.
Values may be sent and summed in bfloat16 or wider, within the bound.
No kernel may reach another device: no remote copies, remote signals or barrier semaphores. Data moves between devices by JAX's collectives and lax.ppermute only.
A program may use at most 64 MiB of HBM per device.

```python
import jax
import jax.numpy as jnp
from jax import lax

D = 4096
FF = 7168
TOKENS = 256
ISLANDS = 4
FRAG = 196608
N_ISLAND = 4
N_TP = 8


def fragment_pair(key):
    base = jax.random.fold_in(key, 7177)
    first, second, third = jax.random.split(base, 3)
    global_values = jnp.clip(jax.random.normal(first, (FRAG,), jnp.float32), -6.0, 6.0)
    common = 0.3 * jnp.clip(jax.random.normal(second, (FRAG,), jnp.float32), -4.0, 4.0)
    own = 0.3 * jnp.clip(jax.random.normal(third, (ISLANDS, FRAG), jnp.float32), -4.0, 4.0)
    local_values = global_values[None, :] - common[None, :] - own
    return (global_values, local_values)


def draw_global_fragment(key, part):
    return fragment_pair(key)[0]


def draw_local_fragment(key, part):
    return fragment_pair(key)[1]


def steps_of(rng, dims, pieces, smallest, largest):
    def one(dim, shards_of):
        draws = jax.random.uniform(jax.random.fold_in(jax.random.fold_in(rng, 6), dim), (shards_of,), jnp.float32, smallest / len(pieces), largest / len(pieces))
        return jnp.repeat(jnp.exp(draws), dims[dim] // shards_of).reshape((-1,) + (1,) * (len(dims) - dim - 1))

    factor_of = one(*pieces[0])
    for cut in pieces[1:]:
        factor_of = factor_of * one(*cut)
    return factor_of


def centred(key, extent, scale, bound, cuts=(), kind=jnp.bfloat16):
    drawn = scale * jax.random.normal(key, extent, jnp.float32)
    if cuts:
        drawn = drawn * steps_of(key, extent, cuts, -0.22, 0.18)
    return jnp.clip(drawn, -bound, bound).astype(kind)


def setup_inputs(seed: int = 0) -> dict:
    key_of = jax.random.split(jax.random.key(seed), 9)
    return {
        "tokens": centred(key_of[0], (ISLANDS, TOKENS, D), 1.0, 6.0, ((0, 4), (1, 8))),
        "cotangent": centred(key_of[1], (ISLANDS, TOKENS, D), 0.25, 1.5, ((0, 4), (1, 8))),
        "gate_weight": centred(key_of[2], (D, FF), D ** -0.5, 0.09375, ((1, 8),)),
        "up_weight": centred(key_of[3], (D, FF), D ** -0.5, 0.09375, ((1, 8),)),
        "down_weight": centred(key_of[4], (FF, D), FF ** -0.5, 0.0625, ((0, 8),)),
        "local_fragment": draw_local_fragment(jax.random.fold_in(key_of[8], 71), 0),
        "global_fragment": draw_global_fragment(jax.random.fold_in(key_of[8], 71), 0),
        "outer_velocity": centred(key_of[7], (FRAG,), 0.5, 3.0, ((0, 8),), jnp.float32),
    }


outer_decay = 0.9
outer_stepsize = 0.7


def island_layer(inputs, gate_weight, up_weight, down_weight):
    tokens, cotangent = inputs
    width = FF // N_TP
    gate_value = jnp.dot(tokens, gate_weight, preferred_element_type=jnp.float32)
    up_value = jnp.dot(tokens, up_weight, preferred_element_type=jnp.float32)
    sigmoid_gate = jax.nn.sigmoid(gate_value)
    hidden = (gate_value * sigmoid_gate * up_value).astype(jnp.bfloat16)
    hidden_groups = hidden.astype(jnp.float32).reshape(TOKENS, N_TP, width)
    down_groups = down_weight.astype(jnp.float32).reshape(N_TP, width, D)
    partial_out = jnp.einsum("tgk,gkd->gtd", hidden_groups, down_groups).astype(jnp.bfloat16)
    layer_out = jnp.sum(partial_out.astype(jnp.float32), axis=0).astype(jnp.bfloat16)
    hidden_grad = jnp.dot(cotangent, down_weight.T, preferred_element_type=jnp.float32)
    up_grad = (hidden_grad * gate_value * sigmoid_gate).astype(jnp.bfloat16)
    gate_grad = (hidden_grad * up_value * sigmoid_gate * (1.0 + gate_value * (1.0 - sigmoid_gate))).astype(jnp.bfloat16)
    gate_groups = gate_grad.astype(jnp.float32).reshape(TOKENS, N_TP, width)
    upgrad_groups = up_grad.astype(jnp.float32).reshape(TOKENS, N_TP, width)
    gate_columns = gate_weight.astype(jnp.float32).reshape(D, N_TP, width)
    up_columns = up_weight.astype(jnp.float32).reshape(D, N_TP, width)
    partial_back = jnp.einsum("tgk,dgk->gtd", gate_groups, gate_columns) + jnp.einsum("tgk,dgk->gtd", upgrad_groups, up_columns)
    partial_back = partial_back.astype(jnp.bfloat16)
    input_grad = jnp.sum(partial_back.astype(jnp.float32), axis=0).astype(jnp.bfloat16)
    return layer_out, input_grad


def reference(tokens, cotangent, gate_weight, up_weight, down_weight, local_fragment, global_fragment, outer_velocity):
    layer_out, input_grad = lax.map(
        lambda pair: island_layer(pair, gate_weight, up_weight, down_weight), (tokens, cotangent))
    difference = global_fragment[None, :] - local_fragment
    average = jnp.sum(difference, axis=0) / N_ISLAND
    new_velocity = outer_decay * outer_velocity + average
    new_fragment = global_fragment - outer_stepsize * (average + outer_decay * new_velocity)
    return layer_out, input_grad, new_fragment, new_velocity
```

```python
import functools

import jax
import jax.numpy as jnp
from jax import lax
from jax.experimental import pallas as pl
from jax.experimental.pallas import tpu as pltpu
from jax.sharding import PartitionSpec as P

outer_decay = 0.9
outer_stepsize = 0.7


F32 = jnp.float32
BF16 = jnp.bfloat16
NT = (((1,), (1,)), ((), ()))
VMEM = pl.BlockSpec(memory_space=pltpu.VMEM)
MIB = 1024 * 1024


def tiles(total, size):
    return [(s, min(size, total - s)) for s in range(0, total, size)]


def call(kernel, name, n_in, outs, flops, limit=8):
    return pl.pallas_call(
        kernel,
        in_specs=[VMEM] * n_in,
        out_specs=[VMEM] * len(outs),
        out_shape=[jax.ShapeDtypeStruct(shape, dtype) for shape, dtype in outs],
        cost_estimate=pl.CostEstimate(flops=flops, bytes_accessed=flops // 256, transcendentals=0),
        compiler_params=pltpu.CompilerParams(vmem_limit_bytes=limit * MIB),
        name=name,
    )


def gateup_kernel(n, *refs):
    blocks = refs[:n]
    gate_ref, up_ref, hidden_ref, silu_ref, slope_ref = refs[n:]
    for s, m in tiles(gate_ref.shape[1], 256):
        x = jnp.concatenate([r[...] for r in blocks], axis=0)
        gate = jnp.dot(x, gate_ref[:, s : s + m], preferred_element_type=F32)
        up = jnp.dot(x, up_ref[:, s : s + m], preferred_element_type=F32)
        sig = jax.nn.sigmoid(gate)
        silu = gate * sig
        hidden_ref[:, s : s + m] = (silu * up).astype(BF16)
        silu_ref[:, s : s + m] = silu
        slope_ref[:, s : s + m] = up * sig * (1.0 + gate * (1.0 - sig))


def gateup(blocks, gate_weight, up_weight):
    rows = sum(b.shape[0] for b in blocks)
    d, w = gate_weight.shape
    return call(
        functools.partial(gateup_kernel, len(blocks)),
        "gateup",
        len(blocks) + 2,
        [((rows, w), BF16), ((rows, w), F32), ((rows, w), F32)],
        4 * rows * d * w,
    )(*blocks, gate_weight, up_weight)


def down_kernel(start, hidden_ref, down_ref, send_ref, keep_ref):
    ns = send_ref.shape[0]
    for s, m in tiles(send_ref.shape[1], 512):
        part = jnp.dot(
            hidden_ref[...], down_ref[:, start + s : start + s + m], preferred_element_type=F32
        ).astype(BF16)
        send_ref[:, s : s + m] = part[:ns]
        keep_ref[:, s : s + m] = part[ns:]


def down(hidden, down_weight, ns, start, cols):
    rows, w = hidden.shape
    return call(
        functools.partial(down_kernel, start),
        "down",
        2,
        [((ns, cols), BF16), ((rows - ns, cols), BF16)],
        2 * rows * cols * w,
    )(hidden, down_weight)


def hgrad_kernel(n, *refs):
    blocks = refs[:n]
    down_ref, silu_ref, slope_ref, up_grad_ref, gate_grad_ref = refs[n:]
    for s, m in tiles(down_ref.shape[0], 256):
        x = jnp.concatenate([r[...] for r in blocks], axis=0)
        h = lax.dot_general(x, down_ref[s : s + m, :], NT, preferred_element_type=F32)
        up_grad_ref[:, s : s + m] = (h * silu_ref[:, s : s + m]).astype(BF16)
        gate_grad_ref[:, s : s + m] = (h * slope_ref[:, s : s + m]).astype(BF16)


def hgrad(blocks, down_weight, silu, slope):
    rows = sum(b.shape[0] for b in blocks)
    w, d = down_weight.shape
    return call(
        functools.partial(hgrad_kernel, len(blocks)),
        "hgrad",
        len(blocks) + 3,
        [((rows, w), BF16), ((rows, w), BF16)],
        2 * rows * d * w,
    )(*blocks, down_weight, silu, slope)


def back_kernel(start, gate_grad_ref, up_grad_ref, gate_ref, up_ref, send_ref, keep_ref):
    ns = send_ref.shape[0]
    for s, m in tiles(send_ref.shape[1], 512):
        at = slice(start + s, start + s + m)
        part = lax.dot_general(gate_grad_ref[...], gate_ref[at, :], NT, preferred_element_type=F32)
        part += lax.dot_general(up_grad_ref[...], up_ref[at, :], NT, preferred_element_type=F32)
        part = part.astype(BF16)
        send_ref[:, s : s + m] = part[:ns]
        keep_ref[:, s : s + m] = part[ns:]


def back(gate_grad, up_grad, gate_weight, up_weight, ns, start, cols):
    rows, w = gate_grad.shape
    return call(
        functools.partial(back_kernel, start),
        "back",
        4,
        [((ns, cols), BF16), ((rows - ns, cols), BF16)],
        4 * rows * cols * w,
    )(gate_grad, up_grad, gate_weight, up_weight)


def add(*terms):
    return sum(t.astype(F32) for t in terms).astype(BF16)


def first_kernel(keep_ref, got_ref, far_ref, one_ref, zero_ref):
    r = far_ref.shape[0]
    zero_ref[...] = add(keep_ref[2 * r : 3 * r], got_ref[r : 2 * r])
    one_ref[...] = add(keep_ref[3 * r : 4 * r], got_ref[2 * r :])
    far_ref[...] = add(keep_ref[4 * r :], got_ref[:r])


def first_sums(keep, got):
    r = got.shape[0] // 3
    cols = got.shape[1]
    return call(first_kernel, "first_sums", 2, [((r, cols), BF16)] * 3, 6 * r * cols)(keep, got)


def pair_kernel(row, keep_ref, got_ref, out_ref):
    r = out_ref.shape[0]
    out_ref[...] = add(keep_ref[row * r : (row + 1) * r], got_ref[...])


def pair_sum(keep, got, row, name):
    return call(functools.partial(pair_kernel, row), name, 2, [(got.shape, BF16)], 2 * got.size)(
        keep, got
    )[0]


def last_kernel(keep_ref, near_ref, core_ref, out_ref):
    r = out_ref.shape[0]
    out_ref[...] = add(keep_ref[:r], near_ref[...], core_ref[...])


def last_sum(keep, near, core):
    return call(last_kernel, "last_sum", 3, [(near.shape, BF16)], 2 * near.size)(keep, near, core)[0]


def moved(axis_of_core):
    pairs = []
    for t in range(8):
        pairs.append((t, t ^ axis_of_core(t & 1)))
    return pairs


SWAP = moved(lambda core: 1)
NEAR = moved(lambda core: 4 if core else 2)
SIDE = moved(lambda core: 2 if core else 4)


def swap(v):
    return lax.ppermute(v, "tp", SWAP)


def near(v):
    return lax.ppermute(v, "tp", NEAR)


def side(v):
    return lax.ppermute(v, "tp", SIDE)


def gather(own):
    mate = swap(own)
    near_own = near(own)
    near_mate = near(mate)
    far_own = side(near_own)
    side_mate = swap(near_own)
    side_own = swap(near_mate)
    far_mate = swap(far_own)
    return [far_mate, side_mate, side_own, own, mate, near_own, near_mate, far_own]


def scatter(send, keep):
    got = swap(send)
    far, one, zero = first_sums(keep, got)
    far_got = side(far)
    one_got = near(one)
    zero = pair_sum(zero, far_got, 0, "zero_sum")
    zero_got = near(zero)
    mate = pair_sum(keep, one_got, 1, "mate_sum")
    return last_sum(keep, zero_got, swap(mate))


def cube_layer(tokens, cotangent, gate_weight, up_weight, down_weight):
    rows, d = tokens.shape
    halves = 1
    cols = d // halves
    token_blocks = gather(tokens)
    cotangent_blocks = gather(cotangent)
    hidden, silu, slope = gateup(token_blocks, gate_weight, up_weight)
    outs = []
    for h in range(halves):
        send, keep = down(hidden, down_weight, 3 * rows, h * cols, cols)
        outs.append(scatter(send, keep))
    up_grad, gate_grad = hgrad(cotangent_blocks, down_weight, silu, slope)
    backs = []
    for h in range(halves):
        send, keep = back(gate_grad, up_grad, gate_weight, up_weight, 3 * rows, h * cols, cols)
        backs.append(scatter(send, keep))
    return jnp.concatenate(outs, axis=1), jnp.concatenate(backs, axis=1)


def plain_layer(tokens, cotangent, gate_weight, up_weight, down_weight):
    gathered = lax.all_gather(tokens, "tp", axis=0, tiled=True)
    cotangent_all = lax.all_gather(cotangent, "tp", axis=0, tiled=True)
    gate = jnp.dot(gathered, gate_weight, preferred_element_type=F32)
    up = jnp.dot(gathered, up_weight, preferred_element_type=F32)
    sig = jax.nn.sigmoid(gate)
    hidden = (gate * sig * up).astype(BF16)
    part = jnp.dot(hidden, down_weight, preferred_element_type=F32)
    layer_out = lax.psum_scatter(part.astype(BF16), "tp", scatter_dimension=0, tiled=True)
    hidden_grad = lax.dot_general(cotangent_all, down_weight, NT, preferred_element_type=F32)
    up_grad = (hidden_grad * gate * sig).astype(BF16)
    gate_grad = (hidden_grad * up * sig * (1.0 + gate * (1.0 - sig))).astype(BF16)
    part = lax.dot_general(gate_grad, gate_weight, NT, preferred_element_type=F32)
    part += lax.dot_general(up_grad, up_weight, NT, preferred_element_type=F32)
    input_grad = lax.psum_scatter(part.astype(BF16), "tp", scatter_dimension=0, tiled=True)
    return layer_out, input_grad


def island_sum(v):
    islands = lax.axis_size("island")
    if islands & (islands - 1):
        return lax.psum(v, "island")
    step = 1
    while step < islands:
        v = v + lax.ppermute(v, "island", [(i, i ^ step) for i in range(islands)])
        step *= 2
    return v


def outer_update(local_fragment, global_fragment, outer_velocity):
    islands = lax.axis_size("island")
    average = island_sum(global_fragment - local_fragment) / islands
    new_velocity = outer_decay * outer_velocity + average
    new_fragment = global_fragment - outer_stepsize * (average + outer_decay * new_velocity)
    return new_fragment, new_velocity


def local(
    tokens,
    cotangent,
    gate_weight,
    up_weight,
    down_weight,
    local_fragment,
    global_fragment,
    outer_velocity,
):
    layer = cube_layer if lax.axis_size("tp") == 8 else plain_layer
    layer_out, input_grad = layer(tokens[0], cotangent[0], gate_weight, up_weight, down_weight)
    new_fragment, new_velocity = outer_update(local_fragment[0], global_fragment, outer_velocity)
    return layer_out[None], input_grad[None], new_fragment, new_velocity


def solution(mesh):
    in_specs = (
        P("island", "tp", None),
        P("island", "tp", None),
        P(None, "tp"),
        P(None, "tp"),
        P("tp", None),
        P("island", "tp"),
        P("tp"),
        P("tp"),
    )
    out_specs = (P("island", "tp", None), P("island", "tp", None), P("tp"), P("tp"))
    return jax.shard_map(local, mesh=mesh, in_specs=in_specs, out_specs=out_specs, check_vma=False)
```
